32 devices in a mesh: section: 2 (over x), dp: 16 (over z, y, core).
Axes of the slice: x: 2, y: 2, z: 4, core: 2. Of those that a mesh axis runs over, the one named last changes fastest.
Arguments:
- grads: bfloat16 [32, 524288], P(('section', 'dp')), parts along dimension 0, may hold values from -6 to 6
- master: float32 [32, 32768], P(('section', 'dp')), parts along dimension 0, may hold values from -30 to 30
- first_moment: float32 [32, 32768], P(('section', 'dp')), parts along dimension 0, may hold values from -0.6 to 0.6
- second_moment: float32 [32, 32768], P(('section', 'dp')), parts along dimension 0, may hold values from 0.005 to 0.05
- perm: int32 [32], P('section'), parts along dimension 0, may hold values from 0 to 15, each once
- bounds: int32 [34], P('section'), parts along dimension 0, may hold values from 0 to 524288, as said below
Outputs:
- new_weights: bfloat16 [1048576], P('section'), parts along dimension 0
- new_master: float32 [32, 32768], P(('section', 'dp')), parts along dimension 0
- new_first: float32 [32, 32768], P(('section', 'dp')), parts along dimension 0
- new_second: float32 [32, 32768], P(('section', 'dp')), parts along dimension 0
- step_taken: float32 [32, 32768], P(('section', 'dp')), parts along dimension 0
The draws below stay inside these ranges and needn't reach their ends.
There are 2 independent parts, one for each index of `section`. The reference program is written for one: setup_inputs(seed, part) draws one part's arguments, and reference() takes and returns one part's arrays. A program takes and returns all parts, laid end to end along the dimension named above; each array names one. Nothing has to cross between parts.
Inputs may be any that keep to these rules, and one draw needn't show every extreme that they name: `perm`: each device index appears exactly once. `bounds`: strictly increasing multiples of 128, the first 0 and the last 524288.
All inputs are finite; a program needn't handle non-finite values.
Results may differ from the reference program's by a relative error of at most 0.0004.
Values may be sent and summed in bfloat16 or wider, within the bound.
A program may use at most 128 MiB of HBM per device.

```python
import math
import jax
import jax.numpy as jnp
from jax import lax

SHARD = 32768
TENSORS = 16
REPLICAS = 16
TOTAL = 524288


def draw_master(key, part):
    noise_key, scale_key = jax.random.split(jax.random.fold_in(key, 11))
    row_pos = jnp.arange(REPLICAS, dtype=jnp.float32)[:, None] / max(REPLICAS - 1, 1)
    base = jnp.clip(jax.random.normal(noise_key, (REPLICAS, SHARD), jnp.float32), -4.0, 4.0)
    spread = math.log(3.0)
    block_scale = jnp.exp(spread * jax.random.uniform(scale_key, (REPLICAS, SHARD // 128, 1), jnp.float32))
    block_scale = jnp.broadcast_to(block_scale, (REPLICAS, SHARD // 128, 128)).reshape(REPLICAS, SHARD)
    rising = jnp.exp(math.log(3.0) * row_pos)
    return (0.25 * base * block_scale * rising).astype(jnp.float32)


def draw_bounds(key, part):
    units = TOTAL // 128
    shuffled = jax.random.permutation(jax.random.fold_in(key, 23), units - 1) + 1
    cuts = jnp.sort(shuffled[:TENSORS - 1]).astype(jnp.int32) * 128
    return jnp.concatenate([jnp.zeros((1,), jnp.int32), cuts, jnp.full((1,), TOTAL, jnp.int32)]).astype(jnp.int32)


def with_spikes(entries, stream_key, source, target, shards_of, factor):
    owner, partner = [(jnp.arange(entries.shape[axis_at]) // (entries.shape[axis_at] // shards_of)).reshape([-1 if axis == axis_at else 1 for axis in range(entries.ndim)]) for axis_at in (source, target)]
    chosen = jax.random.permutation(stream_key, shards_of)[partner]
    strong = (owner == chosen) | (owner == (partner + shards_of // 2) % shards_of)
    return jnp.where(strong, factor * entries, entries)


def level_of(own_key, dims, cuts, least, largest):
    factor_of, own = 1.0, jax.random.fold_in(own_key, 6)
    for dim, blocks in cuts:
        steps = jnp.exp(jax.random.uniform(jax.random.fold_in(own, dim), (blocks,), jnp.float32, least / len(cuts), largest / len(cuts)))
        factor_of = factor_of * jnp.repeat(steps, dims[dim] // blocks).reshape([-1 if axis == dim else 1 for axis in range(len(dims))])
    return factor_of


def centred(rng, shape, scale, most, shards=(), held_as=jnp.bfloat16):
    array = jax.random.normal(rng, shape, jnp.float32) * scale
    if len(shards) > 0:
        array = level_of(rng, shape, shards, -0.22, 0.18) * array
    return jnp.clip(array, min=-most, max=most).astype(held_as)


def bell_draw_with(own_key, dims, scale, bound, cuts, heavy, held_as=jnp.bfloat16):
    entries = scale * jax.random.normal(own_key, dims, jnp.float32)
    if cuts:
        entries = entries * level_of(own_key, dims, cuts, -0.22, 0.18)
    return jnp.clip(with_spikes(entries, jax.random.fold_in(own_key, 3), *heavy), -bound, bound).astype(held_as)


def setup_inputs(seed: int = 0, part: int = 0) -> dict:
    keys = jax.random.split(jax.random.key(seed), 7)
    part_splits = jax.random.split(jax.random.fold_in(keys[6], part), 7)
    grads = bell_draw_with(part_splits[0], (REPLICAS, TOTAL), 1.0, 6.0, ((0, 16),), (0, 1, 16, 2.0))
    master = draw_master(jax.random.fold_in(jax.random.fold_in(keys[6], part), 71), part)
    first_moment = centred(part_splits[2], (REPLICAS, SHARD), 0.1, 0.6, ((0, 16),), jnp.float32)
    second_moment = jnp.clip(jnp.exp(math.log(0.05) - 2.3025851 * jax.random.uniform(part_splits[3], (REPLICAS, SHARD), jnp.float32) ** level_of(part_splits[3], (REPLICAS, SHARD), ((0, 16),), -0.2, 0.2)), 0.005, 0.05)
    perm = jax.random.permutation(part_splits[4], REPLICAS).astype(jnp.int32)
    bounds = draw_bounds(jax.random.fold_in(jax.random.fold_in(keys[6], part), 71), part)
    return dict(grads=grads, master=master, first_moment=first_moment, second_moment=second_moment, perm=perm, bounds=bounds)


beta_first = 0.9
beta_second = 0.999
first_fix = 1.0 - 0.9 ** 10
second_fix = 1.0 - 0.999 ** 10
adam_eps = 1e-06
norm_eps = 1e-06
decay_rate = 0.01
learn_rate = 0.01

def reference(grads, master, first_moment, second_moment, perm, bounds):
    mean_grad = lax.optimization_barrier(jnp.sum(grads.astype(jnp.float32), axis=0)) / REPLICAS
    own_grad = jnp.take(mean_grad.reshape(REPLICAS, SHARD), perm, axis=0)
    new_first = beta_first * first_moment + (1.0 - beta_first) * own_grad
    new_second = beta_second * second_moment + (1.0 - beta_second) * own_grad * own_grad
    direction = new_first / first_fix / (jnp.sqrt(new_second / second_fix) + adam_eps) + decay_rate * master
    positions = perm.astype(jnp.int32)[:, None] * SHARD + jnp.arange(SHARD, dtype=jnp.int32)[None, :]
    tensor_ids = lax.optimization_barrier(jnp.sum((positions[:, :, None] >= bounds[None, None, 1:TENSORS]).astype(jnp.int32), axis=-1)).reshape(-1)
    weight_sq = jax.ops.segment_sum((master * master).reshape(-1), tensor_ids, TENSORS)
    update_sq = jax.ops.segment_sum((direction * direction).reshape(-1), tensor_ids, TENSORS)
    trust_ratio = jnp.sqrt(weight_sq) / (jnp.sqrt(update_sq) + norm_eps)
    step_taken = jnp.take(trust_ratio, tensor_ids).reshape(REPLICAS, SHARD) * direction
    new_master = master - learn_rate * step_taken
    inverse = jnp.argsort(perm)
    new_weights = jnp.take(new_master.astype(jnp.bfloat16), inverse, axis=0).reshape(-1)
    return (new_weights, new_master, new_first, new_second, step_taken)
```

```python
import functools

import jax
import jax.numpy as jnp
from jax import lax
from jax.experimental import pallas as pl
from jax.experimental.pallas import tpu as pltpu
from jax.sharding import PartitionSpec as P

beta_first = 0.9
beta_second = 0.999
first_fix = 1.0 - 0.9**10
second_fix = 1.0 - 0.999**10
adam_eps = 1e-06
norm_eps = 1e-06
decay_rate = 0.01
learn_rate = 0.01

LANES = 128
MESH = pl.DeviceIdType.MESH


def member_of(position, ranges):
    return (position >= ranges[0:1, :]) & (position < ranges[8:9, :])


def tensor_sums(member, entries):
    squares = jnp.sum(entries * entries, axis=1, keepdims=True)
    return jnp.sum(jnp.where(member, squares, 0.0), axis=0, keepdims=True)


def arrange(
    n,
    tensors,
    perm_ref,
    bounds_ref,
    grads_ref,
    master_ref,
    first_ref,
    second_ref,
    blocks_out,
    state_out,
    owner_out,
    ranges_out,
    raw,
    sems,
):
    rows = master_ref.shape[0]
    span = rows * LANES
    loads = []
    for d in range(n):
        start = pl.multiple_of(perm_ref[d] * span, LANES)
        source = grads_ref.at[:, pl.ds(start, span)]
        loads.append(pltpu.make_async_copy(source, raw.at[d], sems.at[d]))
    for i, ref in enumerate((master_ref, first_ref, second_ref)):
        loads.append(pltpu.make_async_copy(ref, state_out.at[i], sems.at[n + i]))
    for load in loads:
        load.start()
    lane = lax.broadcasted_iota(jnp.int32, (8, LANES), 1)
    low = jnp.full((8, LANES), 2**30, jnp.int32)
    high = low
    for t in range(tensors):
        here = lax.rem(lane, LANES // 2) == t
        low = jnp.where(here, bounds_ref[t], low)
        high = jnp.where(here, bounds_ref[t + 1], high)
    ranges_out[0:8, :] = low
    ranges_out[8:16, :] = high
    owner_out[...] = perm_ref[lax.axis_index("dp")] * span + LANES * (
        lax.broadcasted_iota(jnp.int32, (rows, LANES), 0)
    )
    for d in range(n):
        loads[d].wait()
        wide = raw[d].astype(jnp.float32).reshape(rows, LANES)
        blocks_out[d] = wide.astype(jnp.bfloat16)
    for load in loads[n:]:
        load.wait()


def kernel(
    n,
    blocks_ref,
    state,
    owner,
    ranges,
    gathered,
    master_out,
    first_out,
    second_out,
    step_out,
    side_recv,
    pair_send,
    pair_recv,
    keep,
    far_send,
    far_recv,
    stats,
    side_sems,
    pair_sems,
    far_sems,
    stat_send_sem,
    stat_recv_sem,
    ag_far_sems,
    ag_side_sems,
    ag_pair_sems,
):
    units = n // 4
    section = lax.axis_index("section")
    me = lax.axis_index("dp")
    core = lax.rem(me, 2)
    side = lax.rem(me // 2, 2)
    rank = me // 4

    def at(index):
        return (section, index)

    def device_of(r, s, c):
        return r * 4 + s * 2 + c

    pair_id = device_of(rank, side, 1 - core)
    side_id = device_of(rank, 1 - side, core)

    barrier = pltpu.get_barrier_semaphore()

    def greet(j, carry):
        pl.semaphore_signal(
            barrier, inc=1, device_id=at(lax.rem(me + j, n)), device_id_type=MESH
        )
        return carry

    lax.fori_loop(1, n, greet, 0)

    sign = jnp.where(2 * rank < units, units - 1, 1)
    order = [lax.rem(rank + sign * (1 + s), units) for s in range(units)]

    def block_of(d):
        return blocks_ref[d].astype(jnp.float32)

    pl.semaphore_wait(barrier, n - 1)
    side_copies = []
    for s in range(units):
        copy = pltpu.make_async_remote_copy(
            src_ref=blocks_ref.at[pl.ds(device_of(order[s], 1 - side, 0), 2)],
            dst_ref=side_recv.at[s],
            send_sem=side_sems.at[0, s],
            recv_sem=side_sems.at[1, s],
            device_id=at(side_id),
            device_id_type=MESH,
        )
        copy.start()
        side_copies.append(copy)

    half = LANES // 2
    low_half = lax.broadcasted_iota(jnp.int32, (1, LANES), 1) < half
    member = member_of(owner[...], ranges)
    weight_row = tensor_sums(member, state[0])

    pair_copies = []
    far_copies = []
    own_sum = None

    def finish(s):
        pair_copies[s].wait_recv()
        total = keep[s] + pair_recv[s]
        if s == units - 1:
            return total
        far_send[s] = total
        copy = pltpu.make_async_remote_copy(
            src_ref=far_send.at[s],
            dst_ref=far_recv.at[rank],
            send_sem=far_sems.at[0, s],
            recv_sem=far_sems.at[1, rank],
            device_id=at(device_of(order[s], side, core)),
            device_id_type=MESH,
        )
        copy.start()
        far_copies.append(copy)
        return None

    for s in range(units):
        side_copies[s].wait_recv()
        theirs = device_of(order[s], side, 1 - core)
        mine = device_of(order[s], side, core)
        pair_send[s] = block_of(theirs) + side_recv[s, 1 - core].astype(jnp.float32)
        copy = pltpu.make_async_remote_copy(
            src_ref=pair_send.at[s],
            dst_ref=pair_recv.at[s],
            send_sem=pair_sems.at[0, s],
            recv_sem=pair_sems.at[1, s],
            device_id=at(pair_id),
            device_id_type=MESH,
        )
        copy.start()
        pair_copies.append(copy)
        keep[s] = block_of(mine) + side_recv[s, core].astype(jnp.float32)
        if s >= 1:
            finish(s - 1)
    own_sum = finish(units - 1)

    for j in range(1, units):
        source = lax.rem(rank + j, units)
        pltpu.make_async_remote_copy(
            src_ref=far_send.at[0],
            dst_ref=far_recv.at[source],
            send_sem=far_sems.at[0, 0],
            recv_sem=far_sems.at[1, source],
            device_id=at(side_id),
            device_id_type=MESH,
        ).wait_recv()
        own_sum = own_sum + far_recv[source]

    own_grad = own_sum / n
    new_first = beta_first * state[1] + (1.0 - beta_first) * own_grad
    new_second = beta_second * state[2] + (1.0 - beta_second) * own_grad * own_grad
    direction = (
        new_first / first_fix / (jnp.sqrt(new_second / second_fix) + adam_eps)
        + decay_rate * state[0]
    )
    update_row = tensor_sums(member, direction)
    stat = jnp.where(low_half, weight_row, update_row)
    stats[me] = jnp.broadcast_to(stat, (8, LANES))

    def stat_copy(source, target):
        return pltpu.make_async_remote_copy(
            src_ref=stats.at[source, pl.ds(0, 1)],
            dst_ref=stats.at[source, pl.ds(0, 1)],
            send_sem=stat_send_sem.at[target],
            recv_sem=stat_recv_sem.at[source],
            device_id=at(target),
            device_id_type=MESH,
        )

    def tell(j, carry):
        stat_copy(me, lax.rem(me + j, n)).start()
        return carry

    lax.fori_loop(1, n, tell, 0)
    first_out[...] = new_first
    second_out[...] = new_second

    def hear(j, total):
        other = lax.rem(me + j, n)
        stat_copy(other, other).wait_recv()
        return total + stats[other, pl.ds(0, 1)]

    total = lax.fori_loop(1, n, hear, stat)
    trust_ratio = jnp.sqrt(total) / (
        jnp.sqrt(pltpu.roll(total, half, 1)) + norm_eps
    )
    entry_ratio = jnp.sum(
        jnp.where(member & low_half, trust_ratio, 0.0), axis=1, keepdims=True
    )
    step_taken = entry_ratio * direction
    new_master = state[0] - learn_rate * step_taken
    gathered[me] = new_master.astype(jnp.bfloat16)

    def gather_copy(block, sems, slot, target):
        return pltpu.make_async_remote_copy(
            src_ref=gathered.at[block],
            dst_ref=gathered.at[block],
            send_sem=sems.at[0, slot],
            recv_sem=sems.at[1, slot],
            device_id=at(target),
            device_id_type=MESH,
        )

    waits = []
    ag_side = gather_copy(me, ag_side_sems, rank, side_id)
    ag_side.start()
    waits.append(ag_side)
    for s in range(units - 1):
        copy = pltpu.make_async_remote_copy(
            src_ref=gathered.at[me],
            dst_ref=gathered.at[me],
            send_sem=ag_far_sems.at[0, s],
            recv_sem=ag_far_sems.at[1, rank],
            device_id=at(device_of(order[s], side, core)),
            device_id_type=MESH,
        )
        copy.start()
        waits.append(copy)
    ag_pair = gather_copy(me, ag_pair_sems, 2 * rank + side, pair_id)
    ag_pair.start()
    waits.append(ag_pair)
    master_out[...] = new_master
    step_out[...] = step_taken

    for s in reversed(range(units - 1)):
        source = order[s]
        block = device_of(source, side, core)
        gather_copy(block, ag_far_sems, source, side_id).wait_recv()
        copy = gather_copy(block, ag_side_sems, source, side_id)
        copy.start()
        waits.append(copy)
        copy = gather_copy(block, ag_pair_sems, 2 * source + side, pair_id)
        copy.start()
        waits.append(copy)
    for s in reversed(range(units)):
        source = order[s]
        block = device_of(source, 1 - side, core)
        gather_copy(block, ag_side_sems, source, side_id).wait_recv()
        copy = gather_copy(block, ag_pair_sems, 2 * source + 1 - side, pair_id)
        copy.start()
        waits.append(copy)
    for s in reversed(range(units)):
        for y in range(2):
            block = device_of(order[s], y, 1 - core)
            gather_copy(block, ag_pair_sems, 2 * order[s] + y, pair_id).wait_recv()

    for copy in side_copies + pair_copies + far_copies + waits:
        copy.wait_send()

    def told(j, carry):
        target = lax.rem(me + j, n)
        stat_copy(me, target).wait_send()
        return carry

    lax.fori_loop(1, n, told, 0)

def place(n, perm_ref, gathered, *refs):
    held, (weights_out, *outs, sems) = refs[:4], refs[4:]
    rows = gathered.shape[1]
    copies = []
    for d in range(n):
        start = pl.multiple_of(perm_ref[d] * rows, rows)
        target = weights_out.at[pl.ds(start, rows)]
        copies.append(pltpu.make_async_copy(gathered.at[d], target, sems.at[d]))
    for i, (ref, out) in enumerate(zip(held, outs)):
        copies.append(pltpu.make_async_copy(ref, out, sems.at[n + i]))
    for copy in copies:
        copy.start()
    for copy in copies:
        copy.wait()


def solution(mesh):
    n = mesh.shape["dp"]
    units = n // 4

    def per_device(grads, master, first_moment, second_moment, perm, bounds):
        shard = master.shape[1]
        rows = shard // LANES
        tensors = bounds.shape[0] - 1
        block = (rows, LANES)
        f32 = jnp.float32
        hbm_spec = pl.BlockSpec(memory_space=pltpu.HBM)
        vmem_spec = pl.BlockSpec(memory_space=pltpu.VMEM)
        smem_spec = pl.BlockSpec(memory_space=pltpu.SMEM)
        arranged = pl.pallas_call(
            functools.partial(arrange, n, tensors),
            out_shape=[
                jax.ShapeDtypeStruct((n,) + block, jnp.bfloat16),
                jax.ShapeDtypeStruct((3,) + block, f32),
                jax.ShapeDtypeStruct(block, jnp.int32),
                jax.ShapeDtypeStruct((16, LANES), jnp.int32),
            ],
            in_specs=[smem_spec] * 2 + [hbm_spec] * 4,
            out_specs=[vmem_spec] * 4,
            scratch_shapes=[
                pltpu.VMEM((n, 1, shard), jnp.bfloat16),
                pltpu.SemaphoreType.DMA((n + 3,)),
            ],
            compiler_params=pltpu.CompilerParams(vmem_limit_bytes=32 * 1024 * 1024),
        )(
            perm,
            bounds,
            grads,
            master.reshape(block),
            first_moment.reshape(block),
            second_moment.reshape(block),
        )
        outs = pl.pallas_call(
            functools.partial(kernel, n),
            out_shape=[jax.ShapeDtypeStruct((n,) + block, jnp.bfloat16)]
            + [jax.ShapeDtypeStruct(block, f32)] * 4,
            in_specs=[vmem_spec] * 4,
            out_specs=[vmem_spec] * 5,
            scratch_shapes=[
                pltpu.VMEM((units, 2) + block, jnp.bfloat16),
                pltpu.VMEM((units,) + block, f32),
                pltpu.VMEM((units,) + block, f32),
                pltpu.VMEM((units,) + block, f32),
                pltpu.VMEM((units,) + block, f32),
                pltpu.VMEM((units,) + block, f32),
                pltpu.VMEM((n, 8, LANES), f32),
                pltpu.SemaphoreType.DMA((2, units)),
                pltpu.SemaphoreType.DMA((2, units)),
                pltpu.SemaphoreType.DMA((2, units)),
                pltpu.SemaphoreType.DMA((n,)),
                pltpu.SemaphoreType.DMA((n,)),
                pltpu.SemaphoreType.DMA((2, units)),
                pltpu.SemaphoreType.DMA((2, units)),
                pltpu.SemaphoreType.DMA((2, 2 * units)),
            ],
            compiler_params=pltpu.CompilerParams(
                collective_id=0,
                has_side_effects=True,
                vmem_limit_bytes=32 * 1024 * 1024,
            ),
        )(*arranged)
        outs = pl.pallas_call(
            functools.partial(place, n),
            out_shape=[jax.ShapeDtypeStruct((n * rows, LANES), jnp.bfloat16)]
            + [jax.ShapeDtypeStruct(block, f32)] * 4,
            in_specs=[smem_spec] + [vmem_spec] * 5,
            out_specs=[hbm_spec] * 5,
            scratch_shapes=[pltpu.SemaphoreType.DMA((n + 4,))],
            compiler_params=pltpu.CompilerParams(vmem_limit_bytes=32 * 1024 * 1024),
        )(perm, *outs)
        weights = outs[0].reshape(-1)
        return (weights,) + tuple(out.reshape(1, shard) for out in outs[1:])

    return jax.shard_map(
        per_device,
        mesh=mesh,
        in_specs=(
            P(("section", "dp"), None),
            P(("section", "dp"), None),
            P(("section", "dp"), None),
            P(("section", "dp"), None),
            P("section"),
            P("section"),
        ),
        out_specs=(
            P("section"),
            P(("section", "dp"), None),
            P(("section", "dp"), None),
            P(("section", "dp"), None),
            P(("section", "dp"), None),
        ),
        check_vma=False,
    )
```

```python
import functools

import jax
import jax.numpy as jnp
from jax import lax
from jax.experimental import pallas as pl
from jax.experimental.pallas import tpu as pltpu
from jax.sharding import PartitionSpec as P

beta_first = 0.9
beta_second = 0.999
first_fix = 1.0 - 0.9**10
second_fix = 1.0 - 0.999**10
adam_eps = 1e-06
norm_eps = 1e-06
decay_rate = 0.01
learn_rate = 0.01

LANES = 128
VMEM_BYTES = 67043328
MESH = pl.DeviceIdType.MESH


def tensor_sums(member, entries):
    squares = jnp.sum(entries * entries, axis=1, keepdims=True)
    return jnp.sum(jnp.where(member, squares, 0.0), axis=0, keepdims=True)


def kernel(
    n,
    tensors,
    perm_ref,
    bounds_ref,
    grads_ref,
    master_ref,
    first_ref,
    second_ref,
    gathered,
    master_out,
    first_out,
    second_out,
    step_out,
    raw,
    blocks,
    state,
    side_recv,
    pair_send,
    pair_recv,
    keep,
    far_send,
    far_recv,
    stats,
    load_sems,
    side_sems,
    pair_sems,
    far_sems,
    stat_send_sem,
    stat_recv_sem,
    ag_far_sems,
    ag_side_sems,
    ag_pair_sems,
):
    units = n // 4
    rows = master_ref.shape[0]
    span = rows * LANES
    section = lax.axis_index("section")
    me = lax.axis_index("dp")
    core = lax.rem(me, 2)
    side = lax.rem(me // 2, 2)
    rank = me // 4

    def at(index):
        return (section, index)

    def device_of(r, s, c):
        return r * 4 + s * 2 + c

    pair_id = device_of(rank, side, 1 - core)
    side_id = device_of(rank, 1 - side, core)

    barrier = pltpu.get_barrier_semaphore()

    def greet(j, carry):
        pl.semaphore_signal(
            barrier, inc=1, device_id=at(lax.rem(me + j, n)), device_id_type=MESH
        )
        return carry

    lax.fori_loop(1, n, greet, 0)

    loads = []
    for d in range(n):
        source = grads_ref.at[:, pl.ds(d * span, span)]
        loads.append(pltpu.make_async_copy(source, raw.at[d], load_sems.at[d]))
    for i, ref in enumerate((master_ref, first_ref, second_ref)):
        loads.append(pltpu.make_async_copy(ref, state.at[i], load_sems.at[n + i]))
    for load in loads:
        load.start()

    sign = jnp.where(2 * rank < units, units - 1, 1)
    order = [lax.rem(rank + sign * (1 + s), units) for s in range(units)]

    def block_of(d):
        return raw[perm_ref[d]].astype(jnp.float32).reshape(rows, LANES)

    half = LANES // 2
    lane = lax.broadcasted_iota(jnp.int32, (1, LANES), 1)
    low_half = lane < half
    low = jnp.full((1, LANES), 2**30, jnp.int32)
    high = low
    for t in range(tensors):
        here = lax.rem(lane, half) == t
        low = jnp.where(here, bounds_ref[t], low)
        high = jnp.where(here, bounds_ref[t + 1], high)
    position = perm_ref[me] * span + LANES * lax.broadcasted_iota(
        jnp.int32, (rows, LANES), 0
    )
    member = (position >= low) & (position < high)

    for load in loads[:n]:
        load.wait()
    side_copies = []
    for s in range(units):
        for c in range(2):
            block = block_of(device_of(order[s], 1 - side, c))
            blocks[s, c] = block.astype(jnp.bfloat16)
        if s == 0:
            pl.semaphore_wait(barrier, n - 1)
        copy = pltpu.make_async_remote_copy(
            src_ref=blocks.at[s],
            dst_ref=side_recv.at[s],
            send_sem=side_sems.at[0, s],
            recv_sem=side_sems.at[1, s],
            device_id=at(side_id),
            device_id_type=MESH,
        )
        copy.start()
        side_copies.append(copy)

    for load in loads[n:]:
        load.wait()
    weight_row = tensor_sums(member, state[0])

    pair_copies = []
    far_copies = []
    own_sum = None

    def finish(s):
        pair_copies[s].wait_recv()
        total = keep[s] + pair_recv[s]
        if s == units - 1:
            return total
        far_send[s] = total
        copy = pltpu.make_async_remote_copy(
            src_ref=far_send.at[s],
            dst_ref=far_recv.at[rank],
            send_sem=far_sems.at[0, s],
            recv_sem=far_sems.at[1, rank],
            device_id=at(device_of(order[s], side, core)),
            device_id_type=MESH,
        )
        copy.start()
        far_copies.append(copy)
        return None

    for s in range(units):
        side_copies[s].wait_recv()
        theirs = device_of(order[s], side, 1 - core)
        mine = device_of(order[s], side, core)
        pair_send[s] = block_of(theirs) + side_recv[s, 1 - core].astype(jnp.float32)
        copy = pltpu.make_async_remote_copy(
            src_ref=pair_send.at[s],
            dst_ref=pair_recv.at[s],
            send_sem=pair_sems.at[0, s],
            recv_sem=pair_sems.at[1, s],
            device_id=at(pair_id),
            device_id_type=MESH,
        )
        copy.start()
        pair_copies.append(copy)
        keep[s] = block_of(mine) + side_recv[s, core].astype(jnp.float32)
        if s >= 1:
            finish(s - 1)
    own_sum = finish(units - 1)

    for j in range(1, units):
        source = lax.rem(rank + j, units)
        pltpu.make_async_remote_copy(
            src_ref=far_send.at[0],
            dst_ref=far_recv.at[source],
            send_sem=far_sems.at[0, 0],
            recv_sem=far_sems.at[1, source],
            device_id=at(side_id),
            device_id_type=MESH,
        ).wait_recv()
        own_sum = own_sum + far_recv[source]

    own_grad = own_sum / n
    new_first = beta_first * state[1] + (1.0 - beta_first) * own_grad
    new_second = beta_second * state[2] + (1.0 - beta_second) * own_grad * own_grad
    direction = (
        new_first / first_fix / (jnp.sqrt(new_second / second_fix) + adam_eps)
        + decay_rate * state[0]
    )
    update_row = tensor_sums(member, direction)
    stat = jnp.where(low_half, weight_row, update_row)
    stats[me] = jnp.broadcast_to(stat, (8, LANES))

    def stat_copy(source, target):
        return pltpu.make_async_remote_copy(
            src_ref=stats.at[source, pl.ds(0, 1)],
            dst_ref=stats.at[source, pl.ds(0, 1)],
            send_sem=stat_send_sem.at[target],
            recv_sem=stat_recv_sem.at[source],
            device_id=at(target),
            device_id_type=MESH,
        )

    def tell(j, carry):
        stat_copy(me, lax.rem(me + j, n)).start()
        return carry

    lax.fori_loop(1, n, tell, 0)
    first_out[...] = new_first
    second_out[...] = new_second

    def hear(j, total):
        other = lax.rem(me + j, n)
        stat_copy(other, other).wait_recv()
        return total + stats[other, pl.ds(0, 1)]

    total = lax.fori_loop(1, n, hear, stat)
    trust_ratio = jnp.sqrt(total) / (
        jnp.sqrt(pltpu.roll(total, half, 1)) + norm_eps
    )
    entry_ratio = jnp.sum(
        jnp.where(member & low_half, trust_ratio, 0.0), axis=1, keepdims=True
    )
    step_taken = entry_ratio * direction
    new_master = state[0] - learn_rate * step_taken
    gathered[me] = new_master.astype(jnp.bfloat16)

    def gather_copy(block, sems, slot, target):
        return pltpu.make_async_remote_copy(
            src_ref=gathered.at[block],
            dst_ref=gathered.at[block],
            send_sem=sems.at[0, slot],
            recv_sem=sems.at[1, slot],
            device_id=at(target),
            device_id_type=MESH,
        )

    waits = []
    ag_side = gather_copy(me, ag_side_sems, rank, side_id)
    ag_side.start()
    waits.append(ag_side)
    for s in range(units - 1):
        copy = pltpu.make_async_remote_copy(
            src_ref=gathered.at[me],
            dst_ref=gathered.at[me],
            send_sem=ag_far_sems.at[0, s],
            recv_sem=ag_far_sems.at[1, rank],
            device_id=at(device_of(order[s], side, core)),
            device_id_type=MESH,
        )
        copy.start()
        waits.append(copy)
    ag_pair = gather_copy(me, ag_pair_sems, 2 * rank + side, pair_id)
    ag_pair.start()
    waits.append(ag_pair)
    master_out[...] = new_master
    step_out[...] = step_taken

    for s in reversed(range(units - 1)):
        source = order[s]
        block = device_of(source, side, core)
        gather_copy(block, ag_far_sems, source, side_id).wait_recv()
        copy = gather_copy(block, ag_side_sems, source, side_id)
        copy.start()
        waits.append(copy)
        copy = gather_copy(block, ag_pair_sems, 2 * source + side, pair_id)
        copy.start()
        waits.append(copy)
    for s in reversed(range(units)):
        source = order[s]
        block = device_of(source, 1 - side, core)
        gather_copy(block, ag_side_sems, source, side_id).wait_recv()
        copy = gather_copy(block, ag_pair_sems, 2 * source + 1 - side, pair_id)
        copy.start()
        waits.append(copy)
    for s in reversed(range(units)):
        for y in range(2):
            block = device_of(order[s], y, 1 - core)
            gather_copy(block, ag_pair_sems, 2 * order[s] + y, pair_id).wait_recv()

    for copy in side_copies + pair_copies + far_copies + waits:
        copy.wait_send()

    def told(j, carry):
        target = lax.rem(me + j, n)
        stat_copy(me, target).wait_send()
        return carry

    lax.fori_loop(1, n, told, 0)

def place(n, perm_ref, gathered, *refs):
    held, (weights_out, *outs, sems) = refs[:4], refs[4:]
    rows = gathered.shape[1]
    copies = []
    for d in range(n):
        start = pl.multiple_of(perm_ref[d] * rows, rows)
        target = weights_out.at[pl.ds(start, rows)]
        copies.append(pltpu.make_async_copy(gathered.at[d], target, sems.at[d]))
    for i, (ref, out) in enumerate(zip(held, outs)):
        copies.append(pltpu.make_async_copy(ref, out, sems.at[n + i]))
    for copy in copies:
        copy.start()
    for copy in copies:
        copy.wait()


def solution(mesh):
    n = mesh.shape["dp"]
    units = n // 4

    def per_device(grads, master, first_moment, second_moment, perm, bounds):
        shard = master.shape[1]
        rows = shard // LANES
        tensors = bounds.shape[0] - 1
        block = (rows, LANES)
        f32 = jnp.float32
        results = n * shard * 2 + 5 * shard * 4
        hbm_spec = pl.BlockSpec(memory_space=pltpu.HBM)
        vmem_spec = pl.BlockSpec(memory_space=pltpu.VMEM)
        smem_spec = pl.BlockSpec(memory_space=pltpu.SMEM)
        outs = pl.pallas_call(
            functools.partial(kernel, n, tensors),
            out_shape=[jax.ShapeDtypeStruct((n,) + block, jnp.bfloat16)]
            + [jax.ShapeDtypeStruct(block, f32)] * 4,
            in_specs=[smem_spec] * 2 + [hbm_spec] * 4,
            out_specs=[vmem_spec] * 5,
            scratch_shapes=[
                pltpu.VMEM((n, 1, shard), jnp.bfloat16),
                pltpu.VMEM((units, 2) + block, jnp.bfloat16),
                pltpu.VMEM((3,) + block, f32),
                pltpu.VMEM((units, 2) + block, jnp.bfloat16),
                pltpu.VMEM((units,) + block, f32),
                pltpu.VMEM((units,) + block, f32),
                pltpu.VMEM((units,) + block, f32),
                pltpu.VMEM((units,) + block, f32),
                pltpu.VMEM((units,) + block, f32),
                pltpu.VMEM((n, 8, LANES), f32),
                pltpu.SemaphoreType.DMA((n + 3,)),
                pltpu.SemaphoreType.DMA((2, units)),
                pltpu.SemaphoreType.DMA((2, units)),
                pltpu.SemaphoreType.DMA((2, units)),
                pltpu.SemaphoreType.DMA((n,)),
                pltpu.SemaphoreType.DMA((n,)),
                pltpu.SemaphoreType.DMA((2, units)),
                pltpu.SemaphoreType.DMA((2, units)),
                pltpu.SemaphoreType.DMA((2, 2 * units)),
            ],
            compiler_params=pltpu.CompilerParams(
                collective_id=0,
                has_side_effects=True,
                vmem_limit_bytes=VMEM_BYTES - results,
            ),
        )(
            perm,
            bounds,
            grads,
            master.reshape(block),
            first_moment.reshape(block),
            second_moment.reshape(block),
        )
        outs = pl.pallas_call(
            functools.partial(place, n),
            out_shape=[jax.ShapeDtypeStruct((n * rows, LANES), jnp.bfloat16)]
            + [jax.ShapeDtypeStruct(block, f32)] * 4,
            in_specs=[smem_spec] + [vmem_spec] * 5,
            out_specs=[hbm_spec] * 5,
            scratch_shapes=[pltpu.SemaphoreType.DMA((n + 4,))],
            compiler_params=pltpu.CompilerParams(vmem_limit_bytes=32 * 1024 * 1024),
        )(perm, *outs)
        weights = outs[0].reshape(-1)
        return (weights,) + tuple(out.reshape(1, shard) for out in outs[1:])

    return jax.shard_map(
        per_device,
        mesh=mesh,
        in_specs=(
            P(("section", "dp"), None),
            P(("section", "dp"), None),
            P(("section", "dp"), None),
            P(("section", "dp"), None),
            P("section"),
            P("section"),
        ),
        out_specs=(
            P("section"),
            P(("section", "dp"), None),
            P(("section", "dp"), None),
            P(("section", "dp"), None),
            P(("section", "dp"), None),
        ),
        check_vma=False,
    )
```

```python
import functools

import jax
import jax.numpy as jnp
from jax import lax
from jax.experimental import pallas as pl
from jax.experimental.pallas import tpu as pltpu
from jax.sharding import PartitionSpec as P

beta_first = 0.9
beta_second = 0.999
first_fix = 1.0 - 0.9**10
second_fix = 1.0 - 0.999**10
adam_eps = 1e-06
norm_eps = 1e-06
decay_rate = 0.01
learn_rate = 0.01

LANES = 128
VMEM_BYTES = 67043328
MESH = pl.DeviceIdType.MESH


def tensor_sums(member, entries):
    squares = jnp.sum(entries * entries, axis=1, keepdims=True)
    return jnp.sum(jnp.where(member, squares, 0.0), axis=0, keepdims=True)


def kernel(
    n,
    tensors,
    perm_ref,
    bounds_ref,
    grads_ref,
    master_ref,
    first_ref,
    second_ref,
    gathered_out,
    master_out,
    first_out,
    second_out,
    step_out,
    raw,
    blocks,
    state,
    side_recv,
    pair_send,
    pair_recv,
    keep,
    far_send,
    far_recv,
    stats,
    result,
    gathered,
    load_sems,
    store_sems,
    side_sems,
    pair_sems,
    far_sems,
    stat_send_sem,
    stat_recv_sem,
    ag_far_sems,
    ag_side_sems,
    ag_pair_sems,
):
    units = n // 4
    rows = master_ref.shape[0]
    span = rows * LANES
    section = lax.axis_index("section")
    me = lax.axis_index("dp")
    core = lax.rem(me, 2)
    side = lax.rem(me // 2, 2)
    rank = me // 4

    def at(index):
        return (section, index)

    def device_of(r, s, c):
        return r * 4 + s * 2 + c

    pair_id = device_of(rank, side, 1 - core)
    side_id = device_of(rank, 1 - side, core)

    barrier = pltpu.get_barrier_semaphore()

    def greet(j, carry):
        pl.semaphore_signal(
            barrier, inc=1, device_id=at(lax.rem(me + j, n)), device_id_type=MESH
        )
        return carry

    lax.fori_loop(1, n, greet, 0)

    loads = []
    for d in range(n):
        source = grads_ref.at[:, pl.ds(d * span, span)]
        loads.append(pltpu.make_async_copy(source, raw.at[d], load_sems.at[d]))
    for i, ref in enumerate((master_ref, first_ref, second_ref)):
        loads.append(pltpu.make_async_copy(ref, state.at[i], load_sems.at[n + i]))
    for load in loads:
        load.start()

    sign = jnp.where(2 * rank < units, units - 1, 1)
    order = [lax.rem(rank + sign * (1 + s), units) for s in range(units)]

    def block_of(d):
        return raw[perm_ref[d]].astype(jnp.float32).reshape(rows, LANES)

    parts = 2
    depth = rows // parts

    def piece(k):
        return pl.ds(k * depth, depth)

    def part_of(d, k):
        part = raw[perm_ref[d], :, pl.ds(k * depth * LANES, depth * LANES)]
        return part.astype(jnp.float32).reshape(depth, LANES)

    half = LANES // 2
    lane = lax.broadcasted_iota(jnp.int32, (1, LANES), 1)
    low_half = lane < half
    low = jnp.full((1, LANES), 2**30, jnp.int32)
    high = low
    for t in range(tensors):
        here = lax.rem(lane, half) == t
        low = jnp.where(here, bounds_ref[t], low)
        high = jnp.where(here, bounds_ref[t + 1], high)
    position = perm_ref[me] * span + LANES * lax.broadcasted_iota(
        jnp.int32, (rows, LANES), 0
    )
    member = (position >= low) & (position < high)

    for load in loads[:n]:
        load.wait()
    side_copies = []
    for s in range(units):
        for c in range(2):
            block = block_of(device_of(order[s], 1 - side, c))
            blocks[s, c] = block.astype(jnp.bfloat16)
        if s == 0:
            pl.semaphore_wait(barrier, n - 1)
        for k in range(parts):
            copy = pltpu.make_async_remote_copy(
                src_ref=blocks.at[s, :, piece(k)],
                dst_ref=side_recv.at[s, :, piece(k)],
                send_sem=side_sems.at[0, s, k],
                recv_sem=side_sems.at[1, s, k],
                device_id=at(side_id),
                device_id_type=MESH,
            )
            copy.start()
            side_copies.append(copy)

    for load in loads[n:]:
        load.wait()
    weight_row = tensor_sums(member, state[0])

    pair_copies = []
    far_copies = []

    def finish(i):
        s, k = divmod(i, parts)
        pair_copies[i].wait_recv()
        far_send[s, piece(k)] = keep[s, piece(k)] + pair_recv[s, piece(k)]
        if s < units - 1:
            copy = pltpu.make_async_remote_copy(
                src_ref=far_send.at[s, piece(k)],
                dst_ref=far_recv.at[rank, piece(k)],
                send_sem=far_sems.at[0, s, k],
                recv_sem=far_sems.at[1, rank, k],
                device_id=at(device_of(order[s], side, core)),
                device_id_type=MESH,
            )
            copy.start()
            far_copies.append(copy)

    for i in range(units * parts):
        s, k = divmod(i, parts)
        side_copies[i].wait_recv()
        theirs = device_of(order[s], side, 1 - core)
        mine = device_of(order[s], side, core)
        near = side_recv[s, 1 - core, piece(k)].astype(jnp.float32)
        pair_send[s, piece(k)] = part_of(theirs, k) + near
        copy = pltpu.make_async_remote_copy(
            src_ref=pair_send.at[s, piece(k)],
            dst_ref=pair_recv.at[s, piece(k)],
            send_sem=pair_sems.at[0, s, k],
            recv_sem=pair_sems.at[1, s, k],
            device_id=at(pair_id),
            device_id_type=MESH,
        )
        copy.start()
        pair_copies.append(copy)
        near = side_recv[s, core, piece(k)].astype(jnp.float32)
        keep[s, piece(k)] = part_of(mine, k) + near
        if i >= 1:
            finish(i - 1)
    finish(units * parts - 1)
    own_sum = far_send[units - 1]

    for source in order[:-1]:
        for k in range(parts):
            pltpu.make_async_remote_copy(
                src_ref=far_send.at[0, piece(k)],
                dst_ref=far_recv.at[source, piece(k)],
                send_sem=far_sems.at[0, 0, k],
                recv_sem=far_sems.at[1, source, k],
                device_id=at(side_id),
                device_id_type=MESH,
            ).wait_recv()
        own_sum = own_sum + far_recv[source]

    own_grad = own_sum / n
    new_first = beta_first * state[1] + (1.0 - beta_first) * own_grad
    new_second = beta_second * state[2] + (1.0 - beta_second) * own_grad * own_grad
    direction = (
        new_first / first_fix / (jnp.sqrt(new_second / second_fix) + adam_eps)
        + decay_rate * state[0]
    )
    update_row = tensor_sums(member, direction)
    stat = jnp.where(low_half, weight_row, update_row)
    stats[me] = jnp.broadcast_to(stat, (8, LANES))

    def stat_copy(source, target):
        return pltpu.make_async_remote_copy(
            src_ref=stats.at[source, pl.ds(0, 1)],
            dst_ref=stats.at[source, pl.ds(0, 1)],
            send_sem=stat_send_sem.at[target],
            recv_sem=stat_recv_sem.at[source],
            device_id=at(target),
            device_id_type=MESH,
        )

    def tell(j, carry):
        stat_copy(me, lax.rem(me + j, n)).start()
        return carry

    lax.fori_loop(1, n, tell, 0)
    stores = []

    def store(i, value, ref):
        result[i] = value
        copy = pltpu.make_async_copy(result.at[i], ref, store_sems.at[n + i])
        copy.start()
        stores.append(copy)

    def keep_block(d):
        copy = pltpu.make_async_copy(gathered.at[d], gathered_out.at[d], store_sems.at[d])
        copy.start()
        stores.append(copy)

    store(0, new_first, first_out)
    store(1, new_second, second_out)

    def hear(j, total):
        other = lax.rem(me + j, n)
        stat_copy(other, other).wait_recv()
        return total + stats[other, pl.ds(0, 1)]

    total = lax.fori_loop(1, n, hear, stat)
    trust_ratio = jnp.sqrt(total) / (
        jnp.sqrt(pltpu.roll(total, half, 1)) + norm_eps
    )
    entry_ratio = jnp.sum(
        jnp.where(member & low_half, trust_ratio, 0.0), axis=1, keepdims=True
    )
    step_taken = entry_ratio * direction
    new_master = state[0] - learn_rate * step_taken
    gathered[me] = new_master.astype(jnp.bfloat16)

    def gather_copy(block, sems, slot, target):
        return pltpu.make_async_remote_copy(
            src_ref=gathered.at[block],
            dst_ref=gathered.at[block],
            send_sem=sems.at[0, slot],
            recv_sem=sems.at[1, slot],
            device_id=at(target),
            device_id_type=MESH,
        )

    waits = []

    def send(copy):
        copy.start()
        waits.append(copy)

    send(gather_copy(me, ag_side_sems, rank, side_id))
    send(gather_copy(me, ag_pair_sems, 2 * rank + side, pair_id))
    nearest = list(reversed(order[:-1]))
    for s, target in enumerate(nearest):
        send(
            pltpu.make_async_remote_copy(
                src_ref=gathered.at[me],
                dst_ref=gathered.at[me],
                send_sem=ag_far_sems.at[0, s],
                recv_sem=ag_far_sems.at[1, rank],
                device_id=at(device_of(target, side, core)),
                device_id_type=MESH,
            )
        )
    keep_block(me)
    store(2, new_master, master_out)
    store(3, step_taken, step_out)

    def from_far(source):
        block = device_of(source, side, core)
        gather_copy(block, ag_far_sems, source, side_id).wait_recv()
        send(gather_copy(block, ag_side_sems, source, side_id))
        send(gather_copy(block, ag_pair_sems, 2 * source + side, pair_id))
        keep_block(block)

    def from_side(source):
        block = device_of(source, 1 - side, core)
        gather_copy(block, ag_side_sems, source, side_id).wait_recv()
        send(gather_copy(block, ag_pair_sems, 2 * source + 1 - side, pair_id))
        keep_block(block)

    def from_pair(source):
        for y in range(2):
            block = device_of(source, y, 1 - core)
            gather_copy(block, ag_pair_sems, 2 * source + y, pair_id).wait_recv()
            keep_block(block)

    sources = [rank] + nearest
    for s in range(1, units):
        from_far(sources[s])
        from_side(sources[s - 1])
        if s >= 2:
            from_pair(sources[s - 2])
    from_side(sources[-1])
    for source in sources[max(units - 2, 0):]:
        from_pair(source)

    for copy in side_copies + pair_copies + far_copies + waits:
        copy.wait_send()

    def told(j, carry):
        target = lax.rem(me + j, n)
        stat_copy(me, target).wait_send()
        return carry

    lax.fori_loop(1, n, told, 0)
    for copy in stores:
        copy.wait()

def place(n, perm_ref, gathered, *refs):
    held, (weights_out, *outs), (blocks, arrays, sems) = refs[:4], refs[4:9], refs[9:]
    rows = gathered.shape[1]
    loads, stores = [], []
    for d in range(n):
        start = pl.multiple_of(perm_ref[d] * rows, rows)
        target = weights_out.at[pl.ds(start, rows)]
        loads.append(pltpu.make_async_copy(gathered.at[d], blocks.at[d], sems.at[0, d]))
        stores.append(pltpu.make_async_copy(blocks.at[d], target, sems.at[1, d]))
    for i, (ref, out) in enumerate(zip(held, outs)):
        sem = sems.at[0, n + i]
        loads.append(pltpu.make_async_copy(ref, arrays.at[i], sem))
        sem = sems.at[1, n + i]
        stores.append(pltpu.make_async_copy(arrays.at[i], out, sem))
    for load in loads:
        load.start()
    for load, store in zip(loads, stores):
        load.wait()
        store.start()
    for store in stores:
        store.wait()


def solution(mesh):
    n = mesh.shape["dp"]
    units = n // 4

    def per_device(grads, master, first_moment, second_moment, perm, bounds):
        shard = master.shape[1]
        rows = shard // LANES
        tensors = bounds.shape[0] - 1
        block = (rows, LANES)
        f32 = jnp.float32
        hbm_spec = pl.BlockSpec(memory_space=pltpu.HBM)
        smem_spec = pl.BlockSpec(memory_space=pltpu.SMEM)
        outs = pl.pallas_call(
            functools.partial(kernel, n, tensors),
            out_shape=[jax.ShapeDtypeStruct((n,) + block, jnp.bfloat16)]
            + [jax.ShapeDtypeStruct(block, f32)] * 4,
            in_specs=[smem_spec] * 2 + [hbm_spec] * 4,
            out_specs=[hbm_spec] * 5,
            scratch_shapes=[
                pltpu.VMEM((n, 1, shard), jnp.bfloat16),
                pltpu.VMEM((units, 2) + block, jnp.bfloat16),
                pltpu.VMEM((3,) + block, f32),
                pltpu.VMEM((units, 2) + block, jnp.bfloat16),
                pltpu.VMEM((units,) + block, f32),
                pltpu.VMEM((units,) + block, f32),
                pltpu.VMEM((units,) + block, f32),
                pltpu.VMEM((units,) + block, f32),
                pltpu.VMEM((units,) + block, f32),
                pltpu.VMEM((n, 8, LANES), f32),
                pltpu.VMEM((4,) + block, f32),
                pltpu.VMEM((n,) + block, jnp.bfloat16),
                pltpu.SemaphoreType.DMA((n + 3,)),
                pltpu.SemaphoreType.DMA((n + 4,)),
                pltpu.SemaphoreType.DMA((2, units, 2)),
                pltpu.SemaphoreType.DMA((2, units, 2)),
                pltpu.SemaphoreType.DMA((2, units, 2)),
                pltpu.SemaphoreType.DMA((n,)),
                pltpu.SemaphoreType.DMA((n,)),
                pltpu.SemaphoreType.DMA((2, units)),
                pltpu.SemaphoreType.DMA((2, units)),
                pltpu.SemaphoreType.DMA((2, 2 * units)),
            ],
            compiler_params=pltpu.CompilerParams(
                collective_id=0,
                has_side_effects=True,
                vmem_limit_bytes=VMEM_BYTES,
            ),
        )(
            perm,
            bounds,
            grads,
            master.reshape(block),
            first_moment.reshape(block),
            second_moment.reshape(block),
        )
        outs = pl.pallas_call(
            functools.partial(place, n),
            out_shape=[jax.ShapeDtypeStruct((n * rows, LANES), jnp.bfloat16)]
            + [jax.ShapeDtypeStruct(block, f32)] * 4,
            in_specs=[smem_spec] + [hbm_spec] * 5,
            out_specs=[hbm_spec] * 5,
            scratch_shapes=[
                pltpu.VMEM((n,) + block, jnp.bfloat16),
                pltpu.VMEM((4,) + block, f32),
                pltpu.SemaphoreType.DMA((2, n + 4)),
            ],
            compiler_params=pltpu.CompilerParams(vmem_limit_bytes=VMEM_BYTES),
        )(perm, *outs)
        weights = outs[0].reshape(-1)
        return (weights,) + tuple(out.reshape(1, shard) for out in outs[1:])

    return jax.shard_map(
        per_device,
        mesh=mesh,
        in_specs=(
            P(("section", "dp"), None),
            P(("section", "dp"), None),
            P(("section", "dp"), None),
            P(("section", "dp"), None),
            P("section"),
            P("section"),
        ),
        out_specs=(
            P("section"),
            P(("section", "dp"), None),
            P(("section", "dp"), None),
            P(("section", "dp"), None),
            P(("section", "dp"), None),
        ),
        check_vma=False,
    )
```

```python
import functools

import jax
import jax.numpy as jnp
from jax import lax
from jax.experimental import pallas as pl
from jax.experimental.pallas import tpu as pltpu
from jax.sharding import PartitionSpec as P

beta_first = 0.9
beta_second = 0.999
first_fix = 1.0 - 0.9**10
second_fix = 1.0 - 0.999**10
adam_eps = 1e-06
norm_eps = 1e-06
decay_rate = 0.01
learn_rate = 0.01

LANES = 128
VMEM_BYTES = 67043328
PARTS = 4
MESH = pl.DeviceIdType.MESH


def tensor_sums(member, entries):
    squares = jnp.sum(entries * entries, axis=1, keepdims=True)
    return jnp.sum(jnp.where(member, squares, 0.0), axis=0, keepdims=True)


def kernel(
    n,
    tensors,
    perm_ref,
    bounds_ref,
    grads_ref,
    master_ref,
    first_ref,
    second_ref,
    gathered_out,
    master_out,
    first_out,
    second_out,
    step_out,
    raw,
    blocks,
    state,
    side_recv,
    pair_send,
    pair_recv,
    keep,
    far_send,
    far_recv,
    stats,
    result,
    gathered,
    load_sems,
    store_sems,
    side_sems,
    pair_sems,
    far_sems,
    stat_send_sem,
    stat_recv_sem,
    ag_far_sems,
    ag_side_sems,
    ag_pair_sems,
    right_sem,
    left_sem,
):
    units = n // 4
    rows = master_ref.shape[0]
    span = rows * LANES
    section = lax.axis_index("section")
    me = lax.axis_index("dp")
    core = lax.rem(me, 2)
    side = lax.rem(me // 2, 2)
    rank = me // 4

    def at(index):
        return (section, index)

    def device_of(r, s, c):
        return r * 4 + s * 2 + c

    pair_id = device_of(rank, side, 1 - core)
    side_id = device_of(rank, 1 - side, core)

    barrier = pltpu.get_barrier_semaphore()

    def signal(sem, index):
        pl.semaphore_signal(sem, inc=1, device_id=at(index), device_id_type=MESH)

    column = [device_of(rank - 1, side, core), device_of(rank + 1, side, core)]
    has_left, has_right = rank > 0, rank < units - 1
    signal(barrier, pair_id)
    signal(barrier, side_id)
    signal(barrier, device_of(rank, 1 - side, 1 - core))

    @pl.when(has_left)
    def _():
        signal(barrier, column[0])

    @pl.when(has_right)
    def _():
        signal(barrier, column[1])

    def enter():
        sides = jnp.where(has_left & has_right, 2, 1)
        pl.semaphore_wait(barrier, 3 + sides)

    def relay(sem, has_before, has_after, after):
        @pl.when(has_before)
        def _():
            pl.semaphore_wait(sem, 1)

        @pl.when(has_after)
        def _():
            signal(sem, after)

    def enter_all():
        def rightward():
            relay(right_sem, has_left, has_right, column[1])

        def leftward():
            relay(left_sem, has_right, has_left, column[0])

        @pl.when(2 * rank < units)
        def _():
            rightward()
            leftward()

        @pl.when(2 * rank >= units)
        def _():
            leftward()
            rightward()

    loads = []
    for d in range(n):
        source = grads_ref.at[:, pl.ds(d * span, span)]
        loads.append(pltpu.make_async_copy(source, raw.at[d], load_sems.at[d]))
    for i, ref in enumerate((master_ref, first_ref, second_ref)):
        loads.append(pltpu.make_async_copy(ref, state.at[i], load_sems.at[n + i]))
    for load in loads:
        load.start()

    sign = jnp.where(2 * rank < units, units - 1, 1)
    order = [lax.rem(rank + sign * (1 + s), units) for s in range(units)]

    def block_of(d):
        return raw[perm_ref[d]].astype(jnp.float32).reshape(rows, LANES)

    parts = PARTS
    depth = rows // parts

    def piece(k):
        return pl.ds(k * depth, depth)

    def part_of(d, k):
        part = raw[perm_ref[d], :, pl.ds(k * depth * LANES, depth * LANES)]
        return part.astype(jnp.float32).reshape(depth, LANES)

    half = LANES // 2
    lane = lax.broadcasted_iota(jnp.int32, (1, LANES), 1)
    low_half = lane < half
    low = jnp.full((1, LANES), 2**30, jnp.int32)
    high = low
    for t in range(tensors):
        here = lax.rem(lane, half) == t
        low = jnp.where(here, bounds_ref[t], low)
        high = jnp.where(here, bounds_ref[t + 1], high)
    position = perm_ref[me] * span + LANES * lax.broadcasted_iota(
        jnp.int32, (rows, LANES), 0
    )
    member = (position >= low) & (position < high)

    for load in loads[:n]:
        load.wait()
    side_copies = []
    for s in range(units):
        for c in range(2):
            block = block_of(device_of(order[s], 1 - side, c))
            blocks[s, c] = block.astype(jnp.bfloat16)
        if s == 0:
            enter()
        for k in range(parts):
            copy = pltpu.make_async_remote_copy(
                src_ref=blocks.at[s, :, piece(k)],
                dst_ref=side_recv.at[s, :, piece(k)],
                send_sem=side_sems.at[0, s, k],
                recv_sem=side_sems.at[1, s, k],
                device_id=at(side_id),
                device_id_type=MESH,
            )
            copy.start()
            side_copies.append(copy)

    for load in loads[n:]:
        load.wait()
    enter_all()
    weight_row = tensor_sums(member, state[0])

    pair_copies = []
    far_copies = []

    def finish(i):
        s, k = divmod(i, parts)
        pair_copies[i].wait_recv()
        far_send[s, piece(k)] = keep[s, piece(k)] + pair_recv[s, piece(k)]
        if s < units - 1:
            copy = pltpu.make_async_remote_copy(
                src_ref=far_send.at[s, piece(k)],
                dst_ref=far_recv.at[rank, piece(k)],
                send_sem=far_sems.at[0, s, k],
                recv_sem=far_sems.at[1, rank, k],
                device_id=at(device_of(order[s], side, core)),
                device_id_type=MESH,
            )
            copy.start()
            far_copies.append(copy)

    for i in range(units * parts):
        s, k = divmod(i, parts)
        side_copies[i].wait_recv()
        theirs = device_of(order[s], side, 1 - core)
        mine = device_of(order[s], side, core)
        near = side_recv[s, 1 - core, piece(k)].astype(jnp.float32)
        pair_send[s, piece(k)] = part_of(theirs, k) + near
        copy = pltpu.make_async_remote_copy(
            src_ref=pair_send.at[s, piece(k)],
            dst_ref=pair_recv.at[s, piece(k)],
            send_sem=pair_sems.at[0, s, k],
            recv_sem=pair_sems.at[1, s, k],
            device_id=at(pair_id),
            device_id_type=MESH,
        )
        copy.start()
        pair_copies.append(copy)
        near = side_recv[s, core, piece(k)].astype(jnp.float32)
        keep[s, piece(k)] = part_of(mine, k) + near
        if i >= 1:
            finish(i - 1)
    finish(units * parts - 1)
    own_sum = far_send[units - 1]

    for source in order[:-1]:
        for k in range(parts):
            pltpu.make_async_remote_copy(
                src_ref=far_send.at[0, piece(k)],
                dst_ref=far_recv.at[source, piece(k)],
                send_sem=far_sems.at[0, 0, k],
                recv_sem=far_sems.at[1, source, k],
                device_id=at(side_id),
                device_id_type=MESH,
            ).wait_recv()
        own_sum = own_sum + far_recv[source]

    own_grad = own_sum / n
    new_first = beta_first * state[1] + (1.0 - beta_first) * own_grad
    new_second = beta_second * state[2] + (1.0 - beta_second) * own_grad * own_grad
    direction = (
        new_first / first_fix / (jnp.sqrt(new_second / second_fix) + adam_eps)
        + decay_rate * state[0]
    )
    update_row = tensor_sums(member, direction)
    stat = jnp.where(low_half, weight_row, update_row)
    stats[me] = jnp.broadcast_to(stat, (8, LANES))

    def stat_copy(source, target):
        return pltpu.make_async_remote_copy(
            src_ref=stats.at[source, pl.ds(0, 1)],
            dst_ref=stats.at[source, pl.ds(0, 1)],
            send_sem=stat_send_sem.at[target],
            recv_sem=stat_recv_sem.at[source],
            device_id=at(target),
            device_id_type=MESH,
        )

    others = [
        device_of(r, y, c)
        for r in order
        for y in (1 - side, side)
        for c in (1 - core, core)
    ][:-1]
    for other in others:
        stat_copy(me, other).start()
    stores = []

    def store(i, value, ref):
        result[i] = value
        copy = pltpu.make_async_copy(result.at[i], ref, store_sems.at[n + i])
        copy.start()
        stores.append(copy)

    def keep_block(d):
        copy = pltpu.make_async_copy(gathered.at[d], gathered_out.at[d], store_sems.at[d])
        copy.start()
        stores.append(copy)

    store(0, new_first, first_out)
    store(1, new_second, second_out)

    total = stat
    for other in reversed(others):
        stat_copy(other, other).wait_recv()
        total = total + stats[other, pl.ds(0, 1)]
    trust_ratio = jnp.sqrt(total) / (
        jnp.sqrt(pltpu.roll(total, half, 1)) + norm_eps
    )
    entry_ratio = jnp.sum(
        jnp.where(member & low_half, trust_ratio, 0.0), axis=1, keepdims=True
    )
    step_taken = entry_ratio * direction
    new_master = state[0] - learn_rate * step_taken
    gathered[me] = new_master.astype(jnp.bfloat16)

    def gather_copy(block, sems, slot, target):
        return pltpu.make_async_remote_copy(
            src_ref=gathered.at[block],
            dst_ref=gathered.at[block],
            send_sem=sems.at[0, slot],
            recv_sem=sems.at[1, slot],
            device_id=at(target),
            device_id_type=MESH,
        )

    waits = []

    def send(copy):
        copy.start()
        waits.append(copy)

    send(gather_copy(me, ag_side_sems, rank, side_id))
    send(gather_copy(me, ag_pair_sems, 2 * rank + side, pair_id))
    ranked = order[:-1]
    for s, target in enumerate(ranked):
        send(
            pltpu.make_async_remote_copy(
                src_ref=gathered.at[me],
                dst_ref=gathered.at[me],
                send_sem=ag_far_sems.at[0, s],
                recv_sem=ag_far_sems.at[1, rank],
                device_id=at(device_of(target, side, core)),
                device_id_type=MESH,
            )
        )
    keep_block(me)
    store(2, new_master, master_out)
    store(3, step_taken, step_out)

    def from_far(source):
        block = device_of(source, side, core)
        gather_copy(block, ag_far_sems, source, side_id).wait_recv()
        send(gather_copy(block, ag_side_sems, source, side_id))
        send(gather_copy(block, ag_pair_sems, 2 * source + side, pair_id))
        keep_block(block)

    def from_side(source):
        block = device_of(source, 1 - side, core)
        gather_copy(block, ag_side_sems, source, side_id).wait_recv()
        send(gather_copy(block, ag_pair_sems, 2 * source + 1 - side, pair_id))
        keep_block(block)

    def from_pair(source):
        for y in range(2):
            block = device_of(source, y, 1 - core)
            gather_copy(block, ag_pair_sems, 2 * source + y, pair_id).wait_recv()
            keep_block(block)

    sources = [rank] + ranked
    for s in range(1, units):
        from_far(sources[s])
        from_side(sources[s - 1])
        if s >= 2:
            from_pair(sources[s - 2])
    from_side(sources[-1])
    for source in sources[max(units - 2, 0):]:
        from_pair(source)

    for copy in side_copies + pair_copies + far_copies + waits:
        copy.wait_send()

    for other in others:
        stat_copy(me, other).wait_send()
    for copy in stores:
        copy.wait()

def place(n, perm_ref, gathered, *refs):
    held, (weights_out, *outs), (blocks, arrays, sems) = refs[:4], refs[4:9], refs[9:]
    rows = gathered.shape[1]
    loads, stores = [], []
    for d in range(n):
        start = pl.multiple_of(perm_ref[d] * rows, rows)
        target = weights_out.at[pl.ds(start, rows)]
        loads.append(pltpu.make_async_copy(gathered.at[d], blocks.at[d], sems.at[0, d]))
        stores.append(pltpu.make_async_copy(blocks.at[d], target, sems.at[1, d]))
    for i, (ref, out) in enumerate(zip(held, outs)):
        sem = sems.at[0, n + i]
        loads.append(pltpu.make_async_copy(ref, arrays.at[i], sem))
        sem = sems.at[1, n + i]
        stores.append(pltpu.make_async_copy(arrays.at[i], out, sem))
    for load in loads:
        load.start()
    for load, store in zip(loads, stores):
        load.wait()
        store.start()
    for store in stores:
        store.wait()


def solution(mesh):
    n = mesh.shape["dp"]
    units = n // 4

    def per_device(grads, master, first_moment, second_moment, perm, bounds):
        shard = master.shape[1]
        rows = shard // LANES
        tensors = bounds.shape[0] - 1
        block = (rows, LANES)
        f32 = jnp.float32
        hbm_spec = pl.BlockSpec(memory_space=pltpu.HBM)
        smem_spec = pl.BlockSpec(memory_space=pltpu.SMEM)
        outs = pl.pallas_call(
            functools.partial(kernel, n, tensors),
            out_shape=[jax.ShapeDtypeStruct((n,) + block, jnp.bfloat16)]
            + [jax.ShapeDtypeStruct(block, f32)] * 4,
            in_specs=[smem_spec] * 2 + [hbm_spec] * 4,
            out_specs=[hbm_spec] * 5,
            scratch_shapes=[
                pltpu.VMEM((n, 1, shard), jnp.bfloat16),
                pltpu.VMEM((units, 2) + block, jnp.bfloat16),
                pltpu.VMEM((3,) + block, f32),
                pltpu.VMEM((units, 2) + block, jnp.bfloat16),
                pltpu.VMEM((units,) + block, f32),
                pltpu.VMEM((units,) + block, f32),
                pltpu.VMEM((units,) + block, f32),
                pltpu.VMEM((units,) + block, f32),
                pltpu.VMEM((units,) + block, f32),
                pltpu.VMEM((n, 8, LANES), f32),
                pltpu.VMEM((4,) + block, f32),
                pltpu.VMEM((n,) + block, jnp.bfloat16),
                pltpu.SemaphoreType.DMA((n + 3,)),
                pltpu.SemaphoreType.DMA((n + 4,)),
                pltpu.SemaphoreType.DMA((2, units, PARTS)),
                pltpu.SemaphoreType.DMA((2, units, PARTS)),
                pltpu.SemaphoreType.DMA((2, units, PARTS)),
                pltpu.SemaphoreType.DMA((n,)),
                pltpu.SemaphoreType.DMA((n,)),
                pltpu.SemaphoreType.DMA((2, units)),
                pltpu.SemaphoreType.DMA((2, units)),
                pltpu.SemaphoreType.DMA((2, 2 * units)),
                pltpu.SemaphoreType.REGULAR,
                pltpu.SemaphoreType.REGULAR,
            ],
            compiler_params=pltpu.CompilerParams(
                collective_id=0,
                has_side_effects=True,
                vmem_limit_bytes=VMEM_BYTES,
            ),
        )(
            perm,
            bounds,
            grads,
            master.reshape(block),
            first_moment.reshape(block),
            second_moment.reshape(block),
        )
        outs = pl.pallas_call(
            functools.partial(place, n),
            out_shape=[jax.ShapeDtypeStruct((n * rows, LANES), jnp.bfloat16)]
            + [jax.ShapeDtypeStruct(block, f32)] * 4,
            in_specs=[smem_spec] + [hbm_spec] * 5,
            out_specs=[hbm_spec] * 5,
            scratch_shapes=[
                pltpu.VMEM((n,) + block, jnp.bfloat16),
                pltpu.VMEM((4,) + block, f32),
                pltpu.SemaphoreType.DMA((2, n + 4)),
            ],
            compiler_params=pltpu.CompilerParams(vmem_limit_bytes=VMEM_BYTES),
        )(perm, *outs)
        weights = outs[0].reshape(-1)
        return (weights,) + tuple(out.reshape(1, shard) for out in outs[1:])

    return jax.shard_map(
        per_device,
        mesh=mesh,
        in_specs=(
            P(("section", "dp"), None),
            P(("section", "dp"), None),
            P(("section", "dp"), None),
            P(("section", "dp"), None),
            P("section"),
            P("section"),
        ),
        out_specs=(
            P("section"),
            P(("section", "dp"), None),
            P(("section", "dp"), None),
            P(("section", "dp"), None),
            P(("section", "dp"), None),
        ),
        check_vma=False,
    )
```
